32 devices in a mesh: row: 8 (over z, y), col: 4 (over x, core).
Axes of the slice: x: 2, y: 2, z: 4, core: 2. Of those that a mesh axis runs over, the one named last changes fastest.
Arguments:
- matrix_tiles: bfloat16 [8, 4, 96, 256, 256], P('row', 'col'), may hold values from -0.078125 to 0.078125
- tile_rows: int32 [8, 4, 96], P('row', 'col'), may hold values from 0 to 7, as said below
- tile_cols: int32 [8, 4, 96], P('row', 'col'), may hold values from 0 to 15
- tile_count: int32 [8, 4], P('row', 'col'), may hold values from 24 to 96, as said below
- x_start: float32 [16384, 256], P(('col', 'row')), may hold values from -5 to 5
- y_start: float32 [16384, 256], P(('row', 'col')), may hold values from 0 to 1
- cost_vector: float32 [16384, 256], P(('col', 'row')), may hold values from -6 to 6
- right_side: float32 [16384, 256], P(('row', 'col')), may hold values from -6 to 6
- lower_bound: float32 [16384, 256], P(('col', 'row')), may hold values from -1.5 to -0.3
- upper_bound: float32 [16384, 256], P(('col', 'row')), may hold values from 0.3 to 1.5
- step_primal: float32 [256], replicated, may hold values from 0.2 to 0.45
- step_dual: float32 [256], replicated, may hold values from 0.2 to 0.45
Outputs:
- primal_out: float32 [16384, 256], P(('col', 'row'))
- dual_out: float32 [16384, 256], P(('row', 'col'))
The draws below stay inside these ranges and needn't reach their ends.
Inputs may be any that keep to these rules, and one draw needn't show every extreme that they name: Within one grid cell the pairs (tile_rows, tile_cols) of its slots are all different. `tile_count`: some grid cell has 96 used slots in every draw; slots at or above a cell's count are not part of A.
All inputs are finite; a program needn't handle non-finite values.
Results may differ from the reference program's by a relative error of at most 0.001.
Values may be sent and summed in bfloat16 or wider, within the bound.
A program may use at most 128 MiB of HBM per device.

```python
import math
import jax
import jax.numpy as jnp
from jax import lax

TILE = 256
NR_DEV = 8
NC_DEV = 16
TILES_MAX = 96
BATCH = 256
ROWS = 16384
COLS = 16384
N_ROW = 8
N_COL = 4


def tile_places(key):
    key_list = jax.random.split(jax.random.fold_in(key, 7), N_ROW * N_COL)

    def one_cell(cell_key):
        return jax.random.permutation(cell_key, NR_DEV * NC_DEV)[:TILES_MAX]
    shuffled = jax.vmap(one_cell)(key_list)
    return shuffled.reshape(N_ROW, N_COL, TILES_MAX).astype(jnp.int32)


def draw_tile_rows(key, part):
    return (tile_places(key) // NC_DEV).astype(jnp.int32)


def draw_tile_cols(key, part):
    return (tile_places(key) % NC_DEV).astype(jnp.int32)


def draw_tile_count(key, part):
    base_count = jax.random.randint(jax.random.fold_in(key, 3), (N_ROW, N_COL), TILES_MAX // 4, TILES_MAX // 2 + 1)
    heavy_cell = jax.random.randint(jax.random.fold_in(key, 5), (N_ROW, N_COL), 0, 8) == 0
    chosen = jax.random.randint(jax.random.fold_in(key, 9), (), 0, N_ROW * N_COL)
    picked = jnp.arange(N_ROW * N_COL, dtype=jnp.int32).reshape(N_ROW, N_COL) == chosen
    full_count = jnp.full((N_ROW, N_COL), TILES_MAX, jnp.int32)
    return jnp.where(heavy_cell | picked, full_count, base_count).astype(jnp.int32)


def steps_of(own_key, extent, cuts, least, largest):
    def one(position, blocks):
        heights = jax.random.uniform(jax.random.fold_in(jax.random.fold_in(own_key, 6), position), (blocks,), jnp.float32, least / len(cuts), largest / len(cuts))
        return jnp.repeat(jnp.exp(heights), extent[position] // blocks).reshape((-1,) + (1,) * (len(extent) - position - 1))

    factor_of = one(*cuts[0])
    for cut in cuts[1:]:
        factor_of = factor_of * one(*cut)
    return factor_of


def noise(stream_key, dims, width, reach, cuts=(), kind=jnp.bfloat16):
    level = steps_of(stream_key, dims, cuts, -0.22, 0.18) if cuts else 1.0
    entries = jax.random.normal(stream_key, dims, jnp.float32) * width * level
    return jnp.minimum(jnp.maximum(entries, -reach), reach).astype(kind)


def setup_inputs(seed: int = 0) -> dict:
    streams_of = jax.random.split(jax.random.key(seed), 13)
    return {
        "matrix_tiles": noise(streams_of[0], (N_ROW, N_COL, TILES_MAX, TILE, TILE), (TILE * TILES_MAX * N_COL // (2 * NR_DEV)) ** -0.5, 0.078125, ((0, 8), (1, 4))),
        "tile_rows": draw_tile_rows(jax.random.fold_in(streams_of[12], 71), 0),
        "tile_cols": draw_tile_cols(jax.random.fold_in(streams_of[12], 71), 0),
        "tile_count": draw_tile_count(jax.random.fold_in(streams_of[12], 71), 0),
        "x_start": noise(streams_of[4], (COLS, BATCH), 0.8, 5.0, ((0, 32),), jnp.float32),
        "y_start": jnp.clip(1.0 * jax.random.uniform(streams_of[5], (ROWS, BATCH), jnp.float32) ** steps_of(streams_of[5], (ROWS, BATCH), ((0, 32),), -0.2, 0.2), 0.0, 1.0),
        "cost_vector": noise(streams_of[6], (COLS, BATCH), 1.0, 6.0, ((0, 32),), jnp.float32),
        "right_side": noise(streams_of[7], (ROWS, BATCH), 1.0, 6.0, ((0, 32),), jnp.float32),
        "lower_bound": jnp.clip(-1.5 + 1.2 * jax.random.uniform(streams_of[8], (COLS, BATCH), jnp.float32) ** steps_of(streams_of[8], (COLS, BATCH), ((0, 32),), -0.2, 0.2), -1.5, -0.3),
        "upper_bound": jnp.clip(0.3 + 1.2 * jax.random.uniform(streams_of[9], (COLS, BATCH), jnp.float32) ** steps_of(streams_of[9], (COLS, BATCH), ((0, 32),), -0.2, 0.2), 0.3, 1.5),
        "step_primal": jnp.clip(jnp.exp(jax.random.uniform(streams_of[10], (BATCH,), jnp.float32, math.log(0.2), math.log(0.45))), 0.2, 0.45),
        "step_dual": jnp.clip(jnp.exp(jax.random.uniform(streams_of[11], (BATCH,), jnp.float32, math.log(0.2), math.log(0.45))), 0.2, 0.45),
    }


def forward_all(matrix_tiles, tile_rows, tile_cols, tile_count, vector):
    x_tiles = vector.astype(jnp.float32).reshape(N_COL * NC_DEV, TILE, -1)
    slot_ids = jnp.arange(TILES_MAX, dtype=jnp.int32)

    def cell(running, flat):
        grid_row = flat // N_COL
        grid_col = flat % N_COL
        block = matrix_tiles[grid_row, grid_col].astype(jnp.float32)
        pieces = x_tiles[grid_col * NC_DEV + tile_cols[grid_row, grid_col]]
        products = jnp.einsum('sij,sjb->sib', block, pieces, precision=lax.Precision.HIGHEST)
        in_use = slot_ids < tile_count[grid_row, grid_col]
        products = jnp.where(in_use[:, None, None], products, jnp.zeros_like(products))
        running = running.at[grid_row * NR_DEV + tile_rows[grid_row, grid_col]].add(products)
        return (running, None)
    begin = jnp.zeros((N_ROW * NR_DEV, TILE, x_tiles.shape[-1]), jnp.float32)
    total, unused = lax.scan(cell, begin, jnp.arange(N_ROW * N_COL, dtype=jnp.int32))
    return total.reshape(ROWS, -1)

def backward_all(matrix_tiles, tile_rows, tile_cols, tile_count, vector):
    y_tiles = vector.astype(jnp.float32).reshape(N_ROW * NR_DEV, TILE, -1)
    slot_ids = jnp.arange(TILES_MAX, dtype=jnp.int32)

    def cell(running, flat):
        grid_row = flat // N_COL
        grid_col = flat % N_COL
        block = matrix_tiles[grid_row, grid_col].astype(jnp.float32)
        pieces = y_tiles[grid_row * NR_DEV + tile_rows[grid_row, grid_col]]
        products = jnp.einsum('sij,sib->sjb', block, pieces, precision=lax.Precision.HIGHEST)
        in_use = slot_ids < tile_count[grid_row, grid_col]
        products = jnp.where(in_use[:, None, None], products, jnp.zeros_like(products))
        running = running.at[grid_col * NC_DEV + tile_cols[grid_row, grid_col]].add(products)
        return (running, None)
    begin = jnp.zeros((N_COL * NC_DEV, TILE, y_tiles.shape[-1]), jnp.float32)
    total, unused = lax.scan(cell, begin, jnp.arange(N_ROW * N_COL, dtype=jnp.int32))
    return total.reshape(COLS, -1)

def reference(matrix_tiles, tile_rows, tile_cols, tile_count, x_start, y_start, cost_vector, right_side, lower_bound, upper_bound, step_primal, step_dual):
    grad_zero = backward_all(matrix_tiles, tile_rows, tile_cols, tile_count, y_start.astype(jnp.bfloat16))
    primal_one = jnp.clip(x_start - step_primal * (cost_vector - grad_zero), lower_bound, upper_bound)
    ahead_one = (2.0 * primal_one - x_start).astype(jnp.bfloat16)
    image_one = forward_all(matrix_tiles, tile_rows, tile_cols, tile_count, ahead_one)
    dual_one = jnp.maximum(y_start + step_dual * (right_side - image_one), 0.0)
    primal_diff = primal_one - x_start
    dual_diff = dual_one - y_start
    move_primal = lax.optimization_barrier(jnp.sum(primal_diff * primal_diff, axis=0))
    move_dual = lax.optimization_barrier(jnp.sum(dual_diff * dual_diff, axis=0))
    weight = jnp.sqrt((move_dual / ROWS + 1e-06) / (move_primal / COLS + 1e-06))
    grad_one = backward_all(matrix_tiles, tile_rows, tile_cols, tile_count, dual_one.astype(jnp.bfloat16))
    primal_out = jnp.clip(primal_one - step_primal / weight * (cost_vector - grad_one), lower_bound, upper_bound)
    ahead_two = (2.0 * primal_out - primal_one).astype(jnp.bfloat16)
    image_two = forward_all(matrix_tiles, tile_rows, tile_cols, tile_count, ahead_two)
    dual_out = jnp.maximum(dual_one + step_dual * weight * (right_side - image_two), 0.0)
    return (primal_out, dual_out)
```

```python
import jax
import jax.numpy as jnp
from jax import lax
from jax.experimental import pallas as pl
from jax.experimental.pallas import tpu as pltpu
from jax.sharding import PartitionSpec as P

NR_DEV = 8
ZERO_ROWS = 16

eps = 1e-06


def lay_out_kernel(count_ref, rows_ref, cols_ref, tiles_ref, dense_ref, sems):
    edge = tiles_ref.shape[-1]
    count = count_ref[0, 0]

    @pl.loop(0, dense_ref.shape[0] // ZERO_ROWS)
    def _(step):
        at = pl.ds(pl.multiple_of(step * ZERO_ROWS, ZERO_ROWS), ZERO_ROWS)
        dense_ref[at, :] = jnp.zeros((ZERO_ROWS, dense_ref.shape[1]), dense_ref.dtype)

    def copy_of(slot):
        first_row = pl.multiple_of(rows_ref[0, 0, slot] * edge, edge)
        first_col = pl.multiple_of(cols_ref[0, 0, slot] * edge, edge)
        return pltpu.make_async_copy(
            tiles_ref.at[0, 0, slot],
            dense_ref.at[pl.ds(first_row, edge), pl.ds(first_col, edge)],
            sems.at[slot],
        )

    @pl.loop(0, count)
    def _(slot):
        copy_of(slot).start()

    @pl.loop(0, count)
    def _(slot):
        copy_of(slot).wait()


def lay_out(matrix_tiles, tile_rows, tile_cols, tile_count, col_tiles):
    slots, edge = matrix_tiles.shape[2], matrix_tiles.shape[-1]
    shape = (NR_DEV * edge, col_tiles * edge)
    return pl.pallas_call(
        lay_out_kernel,
        out_shape=jax.ShapeDtypeStruct(shape, matrix_tiles.dtype),
        in_specs=[pl.BlockSpec(memory_space=pltpu.SMEM)] * 3
        + [pl.BlockSpec(memory_space=pl.ANY)],
        out_specs=pl.BlockSpec(memory_space=pltpu.VMEM),
        scratch_shapes=[pltpu.SemaphoreType.DMA((slots,))],
        compiler_params=pltpu.CompilerParams(vmem_limit_bytes=40 << 20),
        cost_estimate=pl.CostEstimate(
            flops=0, bytes_accessed=2 * shape[0] * shape[1] * 2, transcendentals=0
        ),
        name="lay_out",
    )(tile_count, tile_rows, tile_cols, matrix_tiles)


def exchange_sum(partial, axis):
    pieces = partial.astype(jnp.bfloat16).reshape(lax.axis_size(axis), -1, partial.shape[-1])
    arrived = lax.all_to_all(pieces, axis, split_axis=0, concat_axis=0, tiled=True)
    return jnp.sum(arrived.astype(jnp.float32), axis=0)


def body(
    matrix_tiles,
    tile_rows,
    tile_cols,
    tile_count,
    x_start,
    y_start,
    cost_seg,
    right_side,
    lower_seg,
    upper_seg,
    step_primal,
    step_dual,
):
    row_devices = lax.axis_size("row")
    col_devices = lax.axis_size("col")
    share = x_start.shape[0]
    edge = matrix_tiles.shape[-1]
    col_tiles = share * row_devices // edge
    total_cols = share * row_devices * col_devices
    total_rows = y_start.shape[0] * row_devices * col_devices
    dense = lay_out(matrix_tiles, tile_rows, tile_cols, tile_count, col_tiles)

    def column_sums(dual):
        segment = lax.all_gather(dual.astype(jnp.bfloat16), "col", axis=0, tiled=True)
        partial = lax.dot_general(
            dense, segment, (((0,), (0,)), ((), ())), preferred_element_type=jnp.float32
        )
        return exchange_sum(partial, "row")

    def row_sums(ahead):
        segment = lax.all_gather(ahead.astype(jnp.bfloat16), "row", axis=0, tiled=True)
        partial = jnp.dot(dense, segment, preferred_element_type=jnp.float32)
        return exchange_sum(partial, "col")

    grad_zero = column_sums(y_start)
    primal_one = jnp.clip(x_start - step_primal * (cost_seg - grad_zero), lower_seg, upper_seg)
    primal_diff = primal_one - x_start
    move_primal = jnp.sum(primal_diff * primal_diff, axis=0)
    image_one = row_sums(2.0 * primal_one - x_start)
    dual_one = jnp.maximum(y_start + step_dual * (right_side - image_one), 0.0)
    dual_diff = dual_one - y_start
    move_dual = jnp.sum(dual_diff * dual_diff, axis=0)
    moves = lax.psum(jnp.stack([move_primal, move_dual]), ("row", "col"))
    weight = jnp.sqrt((moves[1] / total_rows + eps) / (moves[0] / total_cols + eps))
    grad_one = column_sums(dual_one)
    primal_two = jnp.clip(
        primal_one - step_primal / weight * (cost_seg - grad_one), lower_seg, upper_seg
    )
    image_two = row_sums(2.0 * primal_two - primal_one)
    dual_out = jnp.maximum(dual_one + step_dual * weight * (right_side - image_two), 0.0)
    return (primal_two, dual_out)


def solution(mesh):
    placed = (
        P("row", "col", None, None, None),
        P("row", "col", None),
        P("row", "col", None),
        P("row", "col"),
        P(("col", "row"), None),
        P(("row", "col"), None),
        P(("col", "row"), None),
        P(("row", "col"), None),
        P(("col", "row"), None),
        P(("col", "row"), None),
        P(),
        P(),
    )
    return jax.shard_map(
        body,
        mesh=mesh,
        in_specs=placed,
        out_specs=(P(("col", "row"), None), P(("row", "col"), None)),
        check_vma=False,
    )
```

```python
import jax
import jax.numpy as jnp
from jax import lax
from jax.experimental import pallas as pl
from jax.experimental.pallas import tpu as pltpu
from jax.sharding import PartitionSpec as P

NR_DEV = 8
ZERO_ROWS = 16
BATCH_PARTS = 2

eps = 1e-06


def lay_out_kernel(count_ref, rows_ref, cols_ref, tiles_ref, dense_ref, sems):
    edge = tiles_ref.shape[-1]
    count = count_ref[0, 0]

    @pl.loop(0, dense_ref.shape[0] // ZERO_ROWS)
    def _(step):
        at = pl.ds(pl.multiple_of(step * ZERO_ROWS, ZERO_ROWS), ZERO_ROWS)
        dense_ref[at, :] = jnp.zeros((ZERO_ROWS, dense_ref.shape[1]), dense_ref.dtype)

    def copy_of(slot):
        first_row = pl.multiple_of(rows_ref[0, 0, slot] * edge, edge)
        first_col = pl.multiple_of(cols_ref[0, 0, slot] * edge, edge)
        return pltpu.make_async_copy(
            tiles_ref.at[0, 0, slot],
            dense_ref.at[pl.ds(first_row, edge), pl.ds(first_col, edge)],
            sems.at[slot],
        )

    @pl.loop(0, count)
    def _(slot):
        copy_of(slot).start()

    @pl.loop(0, count)
    def _(slot):
        copy_of(slot).wait()


def lay_out(matrix_tiles, tile_rows, tile_cols, tile_count, col_tiles):
    slots, edge = matrix_tiles.shape[2], matrix_tiles.shape[-1]
    shape = (NR_DEV * edge, col_tiles * edge)
    return pl.pallas_call(
        lay_out_kernel,
        out_shape=jax.ShapeDtypeStruct(shape, matrix_tiles.dtype),
        in_specs=[pl.BlockSpec(memory_space=pltpu.SMEM)] * 3
        + [pl.BlockSpec(memory_space=pl.ANY)],
        out_specs=pl.BlockSpec(memory_space=pltpu.VMEM),
        scratch_shapes=[pltpu.SemaphoreType.DMA((slots,))],
        compiler_params=pltpu.CompilerParams(vmem_limit_bytes=40 << 20),
        cost_estimate=pl.CostEstimate(
            flops=0, bytes_accessed=2 * shape[0] * shape[1] * 2, transcendentals=0
        ),
        name="lay_out",
    )(tile_count, tile_rows, tile_cols, matrix_tiles)


def exchange_sum(partial, axis):
    pieces = partial.astype(jnp.bfloat16).reshape(lax.axis_size(axis), -1, partial.shape[-1])
    arrived = lax.all_to_all(pieces, axis, split_axis=0, concat_axis=0, tiled=True)
    return jnp.sum(arrived.astype(jnp.float32), axis=0)


def body(
    matrix_tiles,
    tile_rows,
    tile_cols,
    tile_count,
    x_start,
    y_start,
    cost_seg,
    right_side,
    lower_seg,
    upper_seg,
    step_primal,
    step_dual,
):
    row_devices = lax.axis_size("row")
    col_devices = lax.axis_size("col")
    share = x_start.shape[0]
    edge = matrix_tiles.shape[-1]
    col_tiles = share * row_devices // edge
    total_cols = share * row_devices * col_devices
    total_rows = y_start.shape[0] * row_devices * col_devices
    dense = lay_out(matrix_tiles, tile_rows, tile_cols, tile_count, col_tiles)

    def column_sums(dual):
        segment = lax.all_gather(dual.astype(jnp.bfloat16), "col", axis=0, tiled=True)
        partial = lax.dot_general(
            dense, segment, (((0,), (0,)), ((), ())), preferred_element_type=jnp.float32
        )
        return exchange_sum(partial, "row")

    def row_sums(ahead):
        segment = lax.all_gather(ahead.astype(jnp.bfloat16), "row", axis=0, tiled=True)
        partial = jnp.dot(dense, segment, preferred_element_type=jnp.float32)
        return exchange_sum(partial, "col")

    def iterate(x_start, y_start, cost_seg, right_side, lower_seg, upper_seg, step_primal, step_dual):
        grad_zero = column_sums(y_start)
        primal_one = jnp.clip(x_start - step_primal * (cost_seg - grad_zero), lower_seg, upper_seg)
        primal_diff = primal_one - x_start
        move_primal = jnp.sum(primal_diff * primal_diff, axis=0)
        image_one = row_sums(2.0 * primal_one - x_start)
        dual_one = jnp.maximum(y_start + step_dual * (right_side - image_one), 0.0)
        dual_diff = dual_one - y_start
        move_dual = jnp.sum(dual_diff * dual_diff, axis=0)
        moves = lax.psum(jnp.stack([move_primal, move_dual]), ("row", "col"))
        weight = jnp.sqrt((moves[1] / total_rows + eps) / (moves[0] / total_cols + eps))
        grad_one = column_sums(dual_one)
        primal_two = jnp.clip(
            primal_one - step_primal / weight * (cost_seg - grad_one), lower_seg, upper_seg
        )
        image_two = row_sums(2.0 * primal_two - primal_one)
        dual_out = jnp.maximum(dual_one + step_dual * weight * (right_side - image_two), 0.0)
        return primal_two, dual_out

    arrays = (x_start, y_start, cost_seg, right_side, lower_seg, upper_seg, step_primal, step_dual)
    halves = zip(*(jnp.split(array, BATCH_PARTS, axis=-1) for array in arrays))
    primal_parts, dual_parts = zip(*(iterate(*half) for half in halves))
    return jnp.concatenate(primal_parts, axis=-1), jnp.concatenate(dual_parts, axis=-1)


def solution(mesh):
    placed = (
        P("row", "col", None, None, None),
        P("row", "col", None),
        P("row", "col", None),
        P("row", "col"),
        P(("col", "row"), None),
        P(("row", "col"), None),
        P(("col", "row"), None),
        P(("row", "col"), None),
        P(("col", "row"), None),
        P(("col", "row"), None),
        P(),
        P(),
    )
    return jax.shard_map(
        body,
        mesh=mesh,
        in_specs=placed,
        out_specs=(P(("col", "row"), None), P(("row", "col"), None)),
        check_vma=False,
    )
```
